32 devices in a mesh: seq: 8 (over z, y), chan: 4 (over x, core).
Axes of the slice: x: 2, y: 2, z: 4, core: 2. Of those that a mesh axis runs over, the one named last changes fastest.
Arguments:
- hidden_in: bfloat16 [1024, 2048], P('seq', 'chan'), may hold values from -6 to 6
- norm_gain: float32 [2048], replicated, may hold values from 0.5 to 1.5
- in_weight: bfloat16 [2048, 2, 4096], P('seq', None, 'chan'), may hold values from -0.125 to 0.125
- conv_weight: float32 [2, 4, 4096], P(None, None, 'chan'), may hold values from -3 to 3
- conv_bias: float32 [2, 4096], P(None, 'chan'), may hold values from -0.5 to 0.5
- proj_weight: bfloat16 [2, 4096, 160], P(None, 'chan'), may hold values from -0.1875 to 0.1875
- step_weight: bfloat16 [2, 128, 4096], P(None, None, 'chan'), may hold values from -0.5 to 0.5
- decay_rate: float32 [2, 4096], P(None, 'chan'), may hold values from 0.00024414062 to 0.25
- skip_gain: float32 [2, 4096], P(None, 'chan'), may hold values from 0.5 to 1.5
- out_weight: bfloat16 [4096, 2048], P('chan', 'seq'), may hold values from -0.09375 to 0.09375
Outputs:
- mixed: bfloat16 [1024, 2048], P('seq', 'chan')
The draws below stay inside these ranges and needn't reach their ends.
All inputs are finite; a program needn't handle non-finite values.
Results may differ from the reference program's by a relative error of at most 0.0095.
Values may be sent and summed in bfloat16 or wider, within the bound.
No kernel may reach another device: no remote copies, remote signals or barrier semaphores. Data moves between devices by JAX's collectives and lax.ppermute only.
A program may use at most 128 MiB of HBM per device.

```python
import math
import jax
import jax.numpy as jnp
from jax import lax

D = 2048
E = 4096
STATE = 16
RANK = 128
WIDTH = 4
SEQLEN = 1024


def draw_hidden_in(key, part):
    first_key, second_key = jax.random.split(key, 2)
    direction = jax.random.normal(first_key, (D,), jnp.float32)
    position = jnp.arange(SEQLEN)
    polarity = jnp.where(position < SEQLEN // 2, 1.0, -1.0).astype(jnp.float32)
    random_part = jax.random.normal(second_key, (SEQLEN, D), jnp.float32)
    values = 0.8 * random_part + 0.6 * polarity[:, None] * direction[None, :]
    return jnp.clip(values, -6.0, 6.0).astype(jnp.bfloat16)


def draw_decay_rate(key, part):
    first_key = jax.random.fold_in(key, 0)
    lowest = math.log(0.25 / SEQLEN)
    highest = math.log(0.25)
    logged = jax.random.uniform(first_key, (2, E), jnp.float32, lowest, highest)
    return jnp.exp(logged)


def block_scale(rng, extent, cuts, least, top_value):
    def one(axis_at, parts):
        heights = jax.random.uniform(jax.random.fold_in(jax.random.fold_in(rng, 6), axis_at), (parts,), jnp.float32, least / len(cuts), top_value / len(cuts))
        return jnp.repeat(jnp.exp(heights), extent[axis_at] // parts).reshape((-1,) + (1,) * (len(extent) - axis_at - 1))

    loudness = one(*cuts[0])
    for cut in cuts[1:]:
        loudness = loudness * one(*cut)
    return loudness


def bell_draw(own_key, extent, width, bound, shards=(), dtype=jnp.bfloat16):
    loudness = block_scale(own_key, extent, shards, -0.22, 0.18) if shards else 1.0
    entries = jax.random.normal(own_key, extent, jnp.float32) * width * loudness
    return jnp.minimum(jnp.maximum(entries, -bound), bound).astype(dtype)


def setup_inputs(seed: int = 0) -> dict:
    splits = jax.random.split(jax.random.key(seed), 11)
    hidden_in = draw_hidden_in(jax.random.fold_in(splits[10], 71), 0)
    norm_gain = jnp.clip(1.0 + 0.1 * jax.random.normal(splits[1], (D,), jnp.float32), 0.5, 1.5)
    in_weight = bell_draw(splits[2], (D, 2, E), D ** -0.5, 0.125, ((0, 8), (2, 4)))
    conv_weight = bell_draw(splits[3], (2, WIDTH, E), WIDTH ** -0.5, 3.0, ((2, 4),), jnp.float32)
    conv_bias = jnp.clip(jax.random.uniform(splits[4], (2, E), jnp.float32, -0.5, 0.5) * block_scale(splits[4], (2, E), ((1, 4),), -0.4, 0.0), -0.5, 0.5)
    proj_weight = bell_draw(splits[5], (2, E, 2 * STATE + RANK), (E // 4) ** -0.5, 0.1875, ((1, 4),))
    step_weight = bell_draw(splits[6], (2, RANK, E), RANK ** -0.5, 0.5, ((2, 4),))
    decay_rate = draw_decay_rate(jax.random.fold_in(splits[10], 71), 0)
    skip_gain = jnp.clip(0.5 + 1.0 * jax.random.uniform(splits[8], (2, E), jnp.float32) ** block_scale(splits[8], (2, E), ((1, 4),), -0.2, 0.2), 0.5, 1.5)
    out_weight = bell_draw(splits[9], (E, D), E ** -0.5, 0.09375, ((0, 4), (1, 8)))
    return dict(hidden_in=hidden_in, norm_gain=norm_gain, in_weight=in_weight, conv_weight=conv_weight, conv_bias=conv_bias, proj_weight=proj_weight, step_weight=step_weight, decay_rate=decay_rate, skip_gain=skip_gain, out_weight=out_weight)


def conv_taps(padded, conv_weight, conv_bias, length):
    reach = conv_weight.shape[1] - 1
    forward = jnp.zeros((length, padded.shape[1]), jnp.float32) + conv_bias[0][None, :]
    backward = jnp.zeros((length, padded.shape[1]), jnp.float32) + conv_bias[1][None, :]
    for offset in range(reach + 1):
        forward = forward + conv_weight[0, offset][None, :] * padded[offset:offset + length]
        begin = 2 * reach - offset
        backward = backward + conv_weight[1, offset][None, :] * padded[begin:begin + length]
    return jax.nn.silu(jnp.stack([forward, backward])).astype(jnp.bfloat16)

def sweep_rows(drive_values, key_rows, query_rows, epsilon, reverse):
    start = jnp.zeros((key_rows.shape[1], drive_values.shape[1]), jnp.float32)

    def advance(state, current):
        drive_row, key_row, query_row, eps_row = current
        decay = 1.0 - eps_row[None, :] * (key_row * key_row)[:, None]
        state = decay * state + key_row[:, None] * (eps_row * drive_row)[None, :]
        return (state, lax.optimization_barrier(jnp.sum(query_row[:, None] * state, axis=0)))
    final_state, reads = lax.scan(advance, start, (drive_values, key_rows, query_rows, epsilon), reverse=reverse)
    return reads

def reference(hidden_in, norm_gain, in_weight, conv_weight, conv_bias, proj_weight, step_weight, decay_rate, skip_gain, out_weight):
    hidden = hidden_in.astype(jnp.float32)
    normed = (hidden * lax.rsqrt(lax.optimization_barrier(jnp.mean(hidden * hidden, axis=1, keepdims=True)) + 1e-05) * norm_gain[None, :]).astype(jnp.bfloat16)
    projected = jnp.dot(normed, in_weight.reshape(D, 2 * E), preferred_element_type=jnp.float32).astype(jnp.bfloat16).reshape(SEQLEN, 2, E)
    branch = projected[:, 0, :].astype(jnp.float32)
    gate_half = projected[:, 1, :].astype(jnp.float32)
    padded = jnp.pad(branch, ((WIDTH - 1, WIDTH - 1), (0, 0)))
    driven = conv_taps(padded, conv_weight, conv_bias, SEQLEN)
    drive_values = driven.astype(jnp.float32)
    features = jnp.einsum('dte,def->tdf', drive_values, proj_weight.astype(jnp.float32))
    key_rows = features[:, :, :STATE]
    query_rows = features[:, :, STATE:2 * STATE]
    low_rank = features[:, :, 2 * STATE:].astype(jnp.bfloat16)
    step_size = jnp.einsum('tdr,dre->tde', low_rank.astype(jnp.float32), step_weight.astype(jnp.float32))
    beta_rows = 2.0 * decay_rate[None, :, :] * jax.nn.sigmoid(step_size)
    epsilon = beta_rows / (1.0 + beta_rows * lax.optimization_barrier(jnp.sum(key_rows * key_rows, axis=2, keepdims=True)))
    total = jnp.zeros((SEQLEN, E), jnp.float32)
    for direction in range(2):
        reads = sweep_rows(drive_values[direction], key_rows[:, direction], query_rows[:, direction], epsilon[:, direction], direction == 1)
        total = total + reads + skip_gain[direction][None, :] * drive_values[direction]
    combined = (total * jax.nn.silu(gate_half)).astype(jnp.bfloat16)
    return jnp.dot(combined, out_weight, preferred_element_type=jnp.float32).astype(jnp.bfloat16)
```

```python
import jax
import jax.numpy as jnp
from jax import lax
from jax.experimental import pallas as pl
from jax.experimental.pallas import tpu as pltpu
from jax.sharding import PartitionSpec as P

STATE = 16
WIDTH = 4
LANES = 128
UNROLL = 4


def swap(array, axis, distance):
    count = lax.axis_size(axis)
    return lax.ppermute(array, axis, [(i, i ^ distance) for i in range(count)])


def halo(branch, axis, width):
    count = lax.axis_size(axis)
    forward = [(i, i + 1) for i in range(count - 1)]
    backward = [(target, source) for source, target in forward]
    low = lax.ppermute(branch[:, -width:], axis, forward)
    high = lax.ppermute(branch[:, :width], axis, backward)
    return low, high


def conv_kernel(branch, low, high, weight, bias, proj, driven, features, padded):
    blocks, length, _ = branch.shape
    reach = WIDTH - 1
    first = 8 - reach
    partial = [jnp.zeros(features.shape[1:], jnp.float32) for _ in range(2)]
    for b in range(blocks):
        padded[8 : 8 + length] = branch[b].astype(jnp.float32)
        padded[first:8] = low[b].astype(jnp.float32)
        padded[8 + length : 8 + length + reach] = high[b].astype(jnp.float32)
        for d in range(2):
            total = jnp.broadcast_to(bias[d, b : b + 1], (length, LANES))
            for j in range(WIDTH):
                begin = first + (j if d == 0 else 2 * reach - j)
                total = total + weight[d, j, b : b + 1] * padded[begin : begin + length]
            value = (total / (1.0 + jnp.exp(-total))).astype(jnp.bfloat16)
            driven[d, b] = value
            partial[d] = partial[d] + jnp.dot(
                value, proj[d, b], preferred_element_type=jnp.float32
            )
    for d in range(2):
        features[d] = partial[d]


def spread(target, features, d, start):
    length = features.shape[1]
    for n in range(STATE):
        column = features[d, :, start + n : start + n + 1]
        target[:, n] = jnp.broadcast_to(column, (length, LANES))


def steps(length, reverse, body, carry):
    def many(i, carry):
        for j in range(UNROLL):
            t = i * UNROLL + j
            carry = body(length - 1 - t if reverse else t, carry)
        return carry

    return lax.fori_loop(0, length // UNROLL, many, carry)


def summary_kernel(driven, features, step_weight, rate, eps, drive, product, state, keys):
    _, blocks, length, _ = driven.shape
    for d in range(2):
        key = features[d, :, :STATE]
        square = jnp.sum(key * key, axis=1, keepdims=True)
        low = features[d, :, 2 * STATE :].astype(jnp.bfloat16)
        for b in range(blocks):
            step = jnp.dot(
                low, step_weight[d, :, b * LANES : (b + 1) * LANES],
                preferred_element_type=jnp.float32,
            )
            beta = 2.0 * rate[d, b : b + 1] / (1.0 + jnp.exp(-step))
            value = beta / (1.0 + beta * square)
            eps[d, :, b] = value
            drive[d, :, b] = value * driven[d, b].astype(jnp.float32)
        spread(keys, features, d, 0)

        def body(t, carry):
            products, states = carry
            e, x = eps[d, t], drive[d, t]
            new_products, new_states = [], []
            for n in range(STATE):
                k = jnp.broadcast_to(keys[t, n : n + 1], (blocks, LANES))
                decay = 1.0 - e * (k * k)
                new_products.append(products[n] * decay)
                new_states.append(states[n] * decay + k * x)
            return tuple(new_products), tuple(new_states)

        one = tuple(jnp.ones((blocks, LANES), jnp.float32) for _ in range(STATE))
        zero = tuple(jnp.zeros((blocks, LANES), jnp.float32) for _ in range(STATE))
        products, states = steps(length, d == 1, body, (one, zero))
        for n in range(STATE):
            product[d, n] = products[n].astype(product.dtype)
            state[d, n] = states[n].astype(state.dtype)


def read_kernel(driven, features, eps, drive, initial, gate, skip, out, keys, queries, total):
    _, blocks, length, _ = driven.shape
    for d in range(2):
        spread(keys, features, d, 0)
        spread(queries, features, d, STATE)

        def body(t, states):
            e, x = eps[d, t], drive[d, t]
            new_states = []
            reads = [None] * 4
            for n in range(STATE):
                k = jnp.broadcast_to(keys[t, n : n + 1], (blocks, LANES))
                q = jnp.broadcast_to(queries[t, n : n + 1], (blocks, LANES))
                state = states[n] * (1.0 - e * (k * k)) + k * x
                new_states.append(state)
                part = q * state
                reads[n % 4] = part if reads[n % 4] is None else reads[n % 4] + part
            read = (reads[0] + reads[1]) + (reads[2] + reads[3])
            total[t] = read if d == 0 else total[t] + read
            return tuple(new_states)

        steps(length, d == 1, body, tuple(initial[d, n] for n in range(STATE)))
    for b in range(blocks):
        g = gate[b].astype(jnp.float32)
        reads = total[:, b]
        for d in range(2):
            reads = reads + skip[d, b : b + 1] * driven[d, b].astype(jnp.float32)
        out[:, b * LANES : (b + 1) * LANES] = (reads * (g / (1.0 + jnp.exp(-g)))).astype(
            jnp.bfloat16
        )


def whole(count):
    return [pl.BlockSpec(memory_space=pltpu.VMEM) for _ in range(count)]


def kernel(body, args, shapes, scratch, name):
    return pl.pallas_call(
        body,
        out_shape=[jax.ShapeDtypeStruct(shape, dtype) for shape, dtype in shapes],
        in_specs=whole(len(args)),
        out_specs=whole(len(shapes)),
        scratch_shapes=[pltpu.VMEM(shape, dtype) for shape, dtype in scratch],
        name=name,
    )(*args)


def incoming(product, state):
    count, here = lax.axis_size("seq"), lax.axis_index("seq")
    both = jnp.stack([product, state], 1)
    slots = [None]
    for shift in range(1, count):
        payload = jnp.where(here + shift < count, both[0], both[1])
        slots.append(
            lax.ppermute(payload, "seq", [(i, (i + shift) % count) for i in range(count)])
        )
    result = []
    for d in range(2):
        entering = jnp.zeros(state.shape[1:], jnp.float32)
        passed = jnp.ones(state.shape[1:], jnp.float32)
        for distance in range(1, count):
            slot = slots[distance] if d == 0 else slots[count - distance]
            slot = slot.astype(jnp.float32)
            reached = here >= distance if d == 0 else here + distance < count
            entering = entering + jnp.where(reached, passed * slot[1], 0.0)
            passed = passed * slot[0]
        result.append(entering)
    return jnp.stack(result)


def scatter_sum(partial, axis):
    count, here = lax.axis_size(axis), lax.axis_index(axis)
    rows = partial.shape[0]
    half = 1
    left = count
    parts = partial.reshape(rows, count, -1)
    while left > 1:
        bit = (here // half) % 2
        parts = parts.reshape(rows, left // 2, 2, -1)
        kept = lax.dynamic_index_in_dim(parts, bit, 2, keepdims=False)
        sent = lax.dynamic_index_in_dim(parts, 1 - bit, 2, keepdims=False)
        if left == 2:
            sent = sent.astype(jnp.bfloat16)
        parts = kept + swap(sent, axis, half).astype(jnp.float32)
        half *= 2
        left //= 2
    return parts.reshape(rows, -1)


def per_device(
    hidden_in,
    norm_gain,
    in_weight,
    conv_weight,
    conv_bias,
    proj_weight,
    step_weight,
    decay_rate,
    skip_gain,
    out_weight,
):
    gathered = lax.all_gather(hidden_in, "chan", axis=1, tiled=True).astype(jnp.float32)
    normed = (
        gathered
        * lax.rsqrt(jnp.mean(gathered * gathered, axis=1, keepdims=True) + 1e-05)
        * norm_gain[None, :]
    ).astype(jnp.bfloat16)
    length = normed.shape[0]
    channels = in_weight.shape[2]
    blocks = channels // LANES
    piece = lax.all_gather(in_weight, "seq", axis=0, tiled=True)
    projected = jnp.dot(
        normed, piece.reshape(piece.shape[0], 2 * channels), preferred_element_type=jnp.float32
    ).astype(jnp.bfloat16)
    projected = projected.reshape(length, 2, blocks, LANES).transpose(1, 2, 0, 3)
    branch, gate = projected[0], projected[1]
    low, high = halo(branch, "seq", WIDTH - 1)
    tail = (blocks, LANES)
    bf16, f32 = jnp.bfloat16, jnp.float32
    driven, features = kernel(
        conv_kernel,
        (
            branch,
            low,
            high,
            conv_weight.reshape(2, WIDTH, *tail),
            conv_bias.reshape(2, *tail),
            proj_weight.reshape(2, blocks, LANES, -1),
        ),
        [((2, blocks, length, LANES), bf16), ((2, length, proj_weight.shape[2]), f32)],
        [((length + 16, LANES), f32)],
        "conv",
    )
    distance = 1
    while distance < lax.axis_size("chan"):
        features = features + swap(features, "chan", distance)
        distance *= 2
    spread_shape = ((length, STATE, LANES), f32)
    eps, drive, product, state = kernel(
        summary_kernel,
        (driven, features, step_weight, decay_rate.reshape(2, *tail)),
        [((2, length, *tail), f32)] * 2 + [((2, STATE, *tail), bf16)] * 2,
        [spread_shape],
        "summary",
    )
    initial = incoming(product, state)
    (combined,) = kernel(
        read_kernel,
        (driven, features, eps, drive, initial, gate, skip_gain.reshape(2, *tail)),
        [((length, channels), bf16)],
        [spread_shape] * 2 + [((length, *tail), f32)],
        "read",
    )
    partial_out = jnp.dot(
        combined,
        lax.all_gather(out_weight, "seq", axis=1, tiled=True),
        preferred_element_type=jnp.float32,
    )
    return scatter_sum(partial_out, "chan").astype(jnp.bfloat16)


def solution(mesh):
    in_specs = (
        P("seq", "chan"),
        P(),
        P("seq", None, "chan"),
        P(None, None, "chan"),
        P(None, "chan"),
        P(None, "chan", None),
        P(None, None, "chan"),
        P(None, "chan"),
        P(None, "chan"),
        P("chan", "seq"),
    )
    out_specs = P("seq", "chan")
    return jax.shard_map(
        per_device, mesh=mesh, in_specs=in_specs, out_specs=out_specs, check_vma=False
    )
```

```python
import jax
import jax.numpy as jnp
from jax import lax
from jax.experimental import pallas as pl
from jax.experimental.pallas import tpu as pltpu
from jax.sharding import PartitionSpec as P

STATE = 16
WIDTH = 4
LANES = 128
UNROLL = 4


def swap(array, axis, distance):
    count = lax.axis_size(axis)
    return lax.ppermute(array, axis, [(i, i ^ distance) for i in range(count)])


def halo(slots, axis, width):
    count = lax.axis_size(axis)
    forward = [(i, i + 1) for i in range(count - 1)]
    backward = [(target, source) for source, target in forward]
    first = jnp.concatenate([slot[0, :, :width] for slot in slots])
    last = jnp.concatenate([slot[0, :, -width:] for slot in slots])
    return lax.ppermute(last, axis, forward), lax.ppermute(first, axis, backward)


def project_kernel(place, gain, *refs):
    chans = gain.shape[0]
    hidden, weights, (out, normed) = refs[:chans], refs[chans:-2], refs[-2:]
    slots, length, columns = hidden[0].shape
    rows = weights[0].shape[0]
    shares = columns // rows
    here, chan = place[0], place[1]
    scale = []
    for k in range(slots):
        total = jnp.zeros((length, 1), jnp.float32)
        for part in hidden:
            value = part[k].astype(jnp.float32)
            total = total + jnp.sum(value * value, axis=1, keepdims=True)
        scale.append(lax.rsqrt(total / (columns * chans) + 1e-05))
    for i in range(chans):
        factor = gain[chan ^ i]
        for k in range(slots):
            value = (hidden[i][k].astype(jnp.float32) * scale[k] * factor).astype(jnp.bfloat16)
            for h in range(shares):
                normed[i * shares + h, k * length : (k + 1) * length] = value[
                    :, h * rows : (h + 1) * rows
                ]
    total = None
    for j, weight in enumerate(weights):
        source = here ^ j
        at = ((source // shares) ^ chan) * shares + source % shares
        part = jnp.dot(normed[at], weight[...], preferred_element_type=jnp.float32)
        total = part if total is None else total + part
    _, _, blocks, _, _ = out.shape
    for k in range(slots):
        for p in range(2):
            for h in range(blocks):
                at = (p * blocks + h) * LANES
                out[k, p, h] = total[k * length : (k + 1) * length, at : at + LANES].astype(
                    jnp.bfloat16
                )


def conv_kernel(place, low, high, weight, bias, proj, *refs):
    slots, (driven, gate, features, padded) = refs[:-4], refs[-4:]
    _, blocks, length, _ = slots[0].shape
    count = len(slots)
    reach = WIDTH - 1
    first = 8 - reach
    partial = [jnp.zeros(features.shape[1:], jnp.float32) for _ in range(2)]
    group = place[0] // 2 % count
    below = (place[0] + 2 * count - 1) // 2 % count
    above = (place[0] + 1) // 2 % count
    for k in range(count):
        for h in range(blocks):
            b = (group ^ k) * blocks + h
            padded[8 : 8 + length] = slots[k][0, h].astype(jnp.float32)
            padded[first:8] = low[(group ^ below ^ k) * blocks + h].astype(jnp.float32)
            padded[8 + length : 8 + length + reach] = high[
                (group ^ above ^ k) * blocks + h
            ].astype(jnp.float32)
            gate[b] = slots[k][1, h]
            for d in range(2):
                total = jnp.broadcast_to(bias[d, b], (length, LANES))
                for j in range(WIDTH):
                    begin = first + (j if d == 0 else 2 * reach - j)
                    total = total + weight[d, j, b] * padded[begin : begin + length]
                value = (total / (1.0 + jnp.exp(-total))).astype(jnp.bfloat16)
                driven[d, b] = value
                partial[d] = partial[d] + jnp.dot(
                    value, proj[d, b], preferred_element_type=jnp.float32
                )
    for d in range(2):
        features[d] = partial[d]


def spread(target, features, d, start):
    length = features.shape[1]
    for n in range(STATE):
        column = features[d, :, start + n : start + n + 1]
        target[:, n] = jnp.broadcast_to(column, (length, LANES))


def steps(length, reverse, body, carry):
    def many(i, carry):
        for j in range(UNROLL):
            t = i * UNROLL + j
            carry = body(length - 1 - t if reverse else t, carry)
        return carry

    return lax.fori_loop(0, length // UNROLL, many, carry)


def summary_kernel(driven, features, step_weight, rate, eps, drive, product, state, keys):
    _, blocks, length, _ = driven.shape
    for d in range(2):
        key = features[d, :, :STATE]
        square = jnp.sum(key * key, axis=1, keepdims=True)
        low = features[d, :, 2 * STATE :].astype(jnp.bfloat16)
        for b in range(blocks):
            step = jnp.dot(
                low, step_weight[d, :, b * LANES : (b + 1) * LANES],
                preferred_element_type=jnp.float32,
            )
            beta = 2.0 * rate[d, b : b + 1] / (1.0 + jnp.exp(-step))
            value = beta / (1.0 + beta * square)
            eps[d, :, b] = value
            drive[d, :, b] = value * driven[d, b].astype(jnp.float32)
        spread(keys, features, d, 0)

        def body(t, carry):
            products, states = carry
            e, x = eps[d, t], drive[d, t]
            new_products, new_states = [], []
            for n in range(STATE):
                k = jnp.broadcast_to(keys[t, n : n + 1], (blocks, LANES))
                decay = 1.0 - e * (k * k)
                new_products.append(products[n] * decay)
                new_states.append(states[n] * decay + k * x)
            return tuple(new_products), tuple(new_states)

        one = tuple(jnp.ones((blocks, LANES), jnp.float32) for _ in range(STATE))
        zero = tuple(jnp.zeros((blocks, LANES), jnp.float32) for _ in range(STATE))
        products, states = steps(length, d == 1, body, (one, zero))
        for n in range(STATE):
            product[d, n] = products[n].astype(product.dtype)
            state[d, n] = states[n].astype(state.dtype)


def read_kernel(driven, features, eps, drive, initial, gate, skip, out, keys, queries, total):
    _, blocks, length, _ = driven.shape
    for d in range(2):
        spread(keys, features, d, 0)
        spread(queries, features, d, STATE)

        def body(t, states):
            e, x = eps[d, t], drive[d, t]
            new_states = []
            reads = [None] * 4
            for n in range(STATE):
                k = jnp.broadcast_to(keys[t, n : n + 1], (blocks, LANES))
                q = jnp.broadcast_to(queries[t, n : n + 1], (blocks, LANES))
                state = states[n] * (1.0 - e * (k * k)) + k * x
                new_states.append(state)
                part = q * state
                reads[n % 4] = part if reads[n % 4] is None else reads[n % 4] + part
            read = (reads[0] + reads[1]) + (reads[2] + reads[3])
            total[t] = read if d == 0 else total[t] + read
            return tuple(new_states)

        steps(length, d == 1, body, tuple(initial[d, n] for n in range(STATE)))
    for b in range(blocks):
        g = gate[b].astype(jnp.float32)
        reads = total[:, b]
        for d in range(2):
            reads = reads + skip[d, b : b + 1] * driven[d, b].astype(jnp.float32)
        out[:, b * LANES : (b + 1) * LANES] = (reads * (g / (1.0 + jnp.exp(-g)))).astype(
            jnp.bfloat16
        )


def mix_kernel(place, combined, *refs):
    weights, out = refs[:-1], refs[-1]
    shares = out.shape[1]
    for j, weight in enumerate(weights):
        source = place[0] ^ j
        out[(source // shares) ^ place[1], source % shares] = jnp.dot(
            combined[...], weight[...], preferred_element_type=jnp.float32
        )


def kernel(body, args, shapes, scratch, name):
    return pl.pallas_call(
        body,
        out_shape=[jax.ShapeDtypeStruct(shape, dtype) for shape, dtype in shapes],
        in_specs=[
            pl.BlockSpec(memory_space=pltpu.SMEM if arg.dtype == jnp.int32 else pltpu.VMEM)
            for arg in args
        ],
        out_specs=[pl.BlockSpec(memory_space=pltpu.VMEM) for _ in shapes],
        scratch_shapes=[pltpu.VMEM(shape, dtype) for shape, dtype in scratch],
        name=name,
    )(*args)


def swapped(slots, axis, first, stop):
    distance = stop // 2
    held = {0: slots}
    while distance >= first:
        for at in sorted(held):
            held[at + distance] = swap(held[at], axis, distance)
        distance //= 2
    return [held[at] for at in range(0, stop, first)]


def everywhere(own, others):
    far = [own] + [swap(part, "seq", 2 * (k + 1)) for k, part in enumerate(others)]
    return [part for one in far for part in (one, swap(one, "seq", 1))]


def place():
    return jnp.stack([lax.axis_index("seq"), lax.axis_index("chan")]).astype(jnp.int32)


def exchanged_projection(hidden_in, norm_gain, in_weight):
    seq, chan = lax.axis_size("seq"), lax.axis_size("chan")
    slots = seq // 2
    length, columns = hidden_in.shape
    rows, _, channels = in_weight.shape
    share = channels // slots
    group = lax.axis_index("seq") // 2

    def piece(at):
        part = lax.dynamic_slice_in_dim(in_weight, at * share, share, 2)
        return part.reshape(rows, 2 * share)

    hidden = [hidden_in] + [swap(hidden_in, "seq", 2 * k) for k in range(1, slots)]
    weights = everywhere(piece(group), [piece(group ^ k) for k in range(1, slots)])
    hidden = swapped(jnp.stack(hidden), "chan", 1, chan)
    (projected,) = kernel(
        project_kernel,
        (place(), norm_gain.reshape(chan, 1, columns), *hidden, *weights),
        [((slots, 2, share // LANES, length, LANES), jnp.bfloat16)],
        [((seq * chan * columns // (rows * seq), slots * length, rows), jnp.bfloat16)],
        "project",
    )
    return [projected[0]] + [swap(projected[k], "seq", 2 * k) for k in range(1, slots)]


def gathered_projection(hidden_in, norm_gain, in_weight):
    gathered = lax.all_gather(hidden_in, "chan", axis=1, tiled=True).astype(jnp.float32)
    normed = (
        gathered
        * lax.rsqrt(jnp.mean(gathered * gathered, axis=1, keepdims=True) + 1e-05)
        * norm_gain[None, :]
    ).astype(jnp.bfloat16)
    length = normed.shape[0]
    channels = in_weight.shape[2]
    piece = lax.all_gather(in_weight, "seq", axis=0, tiled=True)
    projected = jnp.dot(
        normed, piece.reshape(piece.shape[0], 2 * channels), preferred_element_type=jnp.float32
    ).astype(jnp.bfloat16)
    return [projected.reshape(length, 2, channels // LANES, LANES).transpose(1, 2, 0, 3)]


def power(count):
    return count & (count - 1) == 0


def incoming(product, state):
    count, here = lax.axis_size("seq"), lax.axis_index("seq")
    both = jnp.stack([product, state], 1)
    slots = [None]
    for shift in range(1, count):
        payload = jnp.where(here + shift < count, both[0], both[1])
        slots.append(
            lax.ppermute(payload, "seq", [(i, (i + shift) % count) for i in range(count)])
        )
    result = []
    for d in range(2):
        entering = jnp.zeros(state.shape[1:], jnp.float32)
        passed = jnp.ones(state.shape[1:], jnp.float32)
        for distance in range(1, count):
            slot = slots[distance] if d == 0 else slots[count - distance]
            slot = slot.astype(jnp.float32)
            reached = here >= distance if d == 0 else here + distance < count
            entering = entering + jnp.where(reached, passed * slot[1], 0.0)
            passed = passed * slot[0]
        result.append(entering)
    return jnp.stack(result)


def exchanged_mix(combined, out_weight):
    seq, chan = lax.axis_size("seq"), lax.axis_size("chan")
    length, columns = combined.shape[0], out_weight.shape[1]
    weights = everywhere(out_weight, [out_weight] * (seq // 2 - 1))
    (partial,) = kernel(
        mix_kernel,
        (place(), combined, *weights),
        [((chan, seq // chan, length, columns), jnp.float32)],
        [],
        "mix",
    )
    parts = [partial[i] for i in range(chan)]
    distance = 1
    while len(parts) > 1:
        sent = jnp.stack(parts[1::2])
        if len(parts) == 2:
            sent = sent.astype(jnp.bfloat16)
        received = swap(sent, "chan", distance).astype(jnp.float32)
        parts = [kept + received[i] for i, kept in enumerate(parts[::2])]
        distance *= 2
    return parts[0].transpose(1, 0, 2).reshape(length, -1).astype(jnp.bfloat16)


def gathered_mix(combined, out_weight):
    partial = jnp.dot(
        combined,
        lax.all_gather(out_weight, "seq", axis=1, tiled=True),
        preferred_element_type=jnp.float32,
    )
    summed = lax.psum(partial, "chan")
    share = summed.shape[1] // lax.axis_size("chan")
    part = lax.dynamic_slice_in_dim(summed, lax.axis_index("chan") * share, share, 1)
    return part.astype(jnp.bfloat16)


def per_device(
    hidden_in,
    norm_gain,
    in_weight,
    conv_weight,
    conv_bias,
    proj_weight,
    step_weight,
    decay_rate,
    skip_gain,
    out_weight,
):
    seq, chan = lax.axis_size("seq"), lax.axis_size("chan")
    length, columns = hidden_in.shape
    rows, _, channels = in_weight.shape
    blocks = channels // LANES
    exchange = (
        power(seq)
        and power(chan)
        and 2 * channels % (seq * LANES) == 0
        and columns % rows == 0
        and rows % LANES == 0
        and seq % chan == 0
    )
    project = exchanged_projection if exchange else gathered_projection
    slots = project(hidden_in, norm_gain, in_weight)
    low, high = halo(slots, "seq", WIDTH - 1)
    tail = (blocks, LANES)
    bf16, f32 = jnp.bfloat16, jnp.float32
    driven, gate, features = kernel(
        conv_kernel,
        (
            lax.axis_index("seq").reshape(1).astype(jnp.int32),
            low,
            high,
            conv_weight.reshape(2, WIDTH, blocks, 1, LANES),
            conv_bias.reshape(2, blocks, 1, LANES),
            proj_weight.reshape(2, blocks, LANES, -1),
            *slots,
        ),
        [
            ((2, blocks, length, LANES), bf16),
            ((blocks, length, LANES), bf16),
            ((2, length, proj_weight.shape[2]), f32),
        ],
        [((length + 16, LANES), f32)],
        "conv",
    )
    distance = 1
    while distance < lax.axis_size("chan"):
        features = features + swap(features, "chan", distance)
        distance *= 2
    spread_shape = ((length, STATE, LANES), f32)
    eps, drive, product, state = kernel(
        summary_kernel,
        (driven, features, step_weight, decay_rate.reshape(2, *tail)),
        [((2, length, *tail), f32)] * 2 + [((2, STATE, *tail), bf16)] * 2,
        [spread_shape],
        "summary",
    )
    initial = incoming(product, state)
    (combined,) = kernel(
        read_kernel,
        (driven, features, eps, drive, initial, gate, skip_gain.reshape(2, *tail)),
        [((length, channels), bf16)],
        [spread_shape] * 2 + [((length, *tail), f32)],
        "read",
    )
    mix = exchanged_mix if exchange else gathered_mix
    return mix(combined, out_weight)


def solution(mesh):
    in_specs = (
        P("seq", "chan"),
        P(),
        P("seq", None, "chan"),
        P(None, None, "chan"),
        P(None, "chan"),
        P(None, "chan", None),
        P(None, None, "chan"),
        P(None, "chan"),
        P(None, "chan"),
        P("chan", "seq"),
    )
    out_specs = P("seq", "chan")
    return jax.shard_map(
        per_device, mesh=mesh, in_specs=in_specs, out_specs=out_specs, check_vma=False
    )
```

```python
import jax
import jax.numpy as jnp
from jax import lax
from jax.experimental import pallas as pl
from jax.experimental.pallas import tpu as pltpu
from jax.sharding import PartitionSpec as P


STATE = 16
WIDTH = 4
LANES = 128
UNROLL = 4
EDGE = 16


def swap(array, axis, distance):
    count = lax.axis_size(axis)
    return lax.ppermute(array, axis, [(i, i ^ distance) for i in range(count)])


def with_edges(branch, axis, width):
    count = lax.axis_size(axis)
    forward = [(i, i + 1) for i in range(count - 1)]
    backward = [(target, source) for source, target in forward]
    low = lax.ppermute(branch[:, -width:], axis, forward)
    high = lax.ppermute(branch[:, :width], axis, backward)
    rest = jnp.zeros((branch.shape[0], EDGE - 2 * width, LANES), branch.dtype)
    return jnp.concatenate([branch, high, low, rest], 1)


def project_kernel(place, gain, *refs):
    chans = gain.shape[0]
    slots, rows_each, columns = refs[0].shape
    hidden, (normed, edges) = refs[:chans], refs[-2:]
    weights, out = refs[chans : -2 - slots], refs[-2 - slots : -2]
    length = rows_each - EDGE
    rows = weights[0].shape[0]
    shares = columns // rows
    here, chan = place[0], place[1]
    scale = []
    for k in range(slots):
        total = jnp.zeros((rows_each, 1), jnp.float32)
        for part in hidden:
            value = part[k].astype(jnp.float32)
            total = total + jnp.sum(value * value, axis=1, keepdims=True)
        scale.append(lax.rsqrt(total / (columns * chans) + 1e-05))
    for i in range(chans):
        factor = gain[chan ^ i]
        for k in range(slots):
            value = (hidden[i][k].astype(jnp.float32) * scale[k] * factor).astype(jnp.bfloat16)
            for h in range(shares):
                normed[i * shares + h, k * rows_each : (k + 1) * rows_each] = value[
                    :, h * rows : (h + 1) * rows
                ]
    total = None
    for j, weight in enumerate(weights):
        source = here ^ j
        at = ((source // shares) ^ chan) * shares + source % shares
        part = jnp.dot(normed[at], weight[...], preferred_element_type=jnp.float32)
        total = part if total is None else total + part
    _, blocks, _, _ = out[0].shape
    for k in range(slots):
        for h in range(blocks):
            edges[k, h] = total[
                k * rows_each + length : (k + 1) * rows_each, h * LANES : (h + 1) * LANES
            ]
        for p in range(2):
            for h in range(blocks):
                at = (p * blocks + h) * LANES
                out[k][p, h, :length] = total[
                    k * rows_each : k * rows_each + length, at : at + LANES
                ].astype(jnp.bfloat16)
    group, side = here // 2, here % 2
    firsts = lax.broadcasted_iota(jnp.int32, (EDGE, LANES), 0) < WIDTH - 1
    for k in range(slots):
        target = group ^ k
        beyond = target + 2 * side - 1
        inside = jnp.logical_and(beyond >= 0, beyond < slots)
        at = group ^ jnp.clip(beyond, 0, slots - 1)
        for h in range(blocks):
            near = edges[k, h]
            far = jnp.where(inside, edges[at, h], 0.0)
            value = jnp.where(firsts == (side == 0), near, far).astype(jnp.bfloat16)
            out[k][0, h, length:] = value
            out[k][1, h, length:] = value


def conv_kernel(place, weight, bias, proj, *refs):
    slots, (driven, gate, features, padded) = refs[:-4], refs[-4:]
    _, blocks, length, _ = slots[0].shape
    length = length - EDGE
    count = len(slots)
    reach = WIDTH - 1
    first = 8 - reach
    partial = [jnp.zeros(features.shape[1:], jnp.float32) for _ in range(2)]
    for k in range(count):
        for h in range(blocks):
            b = (place[0] // 2 % count ^ k) * blocks + h
            lanes = pl.ds(pl.multiple_of(b * LANES, LANES), LANES)
            padded[8 : 8 + length] = slots[k][0, h, :length].astype(jnp.float32)
            beyond = slots[k][0, h, length:].astype(jnp.float32)
            padded[8 + length : 8 + length + reach] = beyond[:reach]
            padded[first:8] = beyond[reach : 2 * reach]
            gate[b] = slots[k][1, h, :length]
            for d in range(2):
                total = jnp.broadcast_to(bias[d : d + 1, lanes], (length, LANES))
                for j in range(WIDTH):
                    begin = first + (j if d == 0 else 2 * reach - j)
                    total = total + weight[d, j : j + 1, lanes] * padded[begin : begin + length]
                value = (total / (1.0 + jnp.exp(-total))).astype(jnp.bfloat16)
                driven[d, b] = value
                partial[d] = partial[d] + jnp.dot(
                    value, proj[d, lanes], preferred_element_type=jnp.float32
                )
    for d in range(2):
        features[d] = partial[d]


def spread(target, features, start):
    length = features.shape[0]
    for n in range(STATE):
        target[n] = jnp.broadcast_to(features[:, start + n : start + n + 1], (length, LANES))


def steps(length, reverse, body, carry):
    def many(i, carry):
        for j in range(UNROLL):
            t = i * UNROLL + j
            carry = body(length - 1 - t if reverse else t, carry)
        return carry

    return lax.fori_loop(0, length // UNROLL, many, carry)


def row(ref, n, t, blocks):
    return jnp.broadcast_to(ref[n, pl.ds(t, 1)], (blocks, LANES))


def summary_kernel(place, driven, here, there, step_weight, rate, eps, drive, *refs):
    payloads, keys = refs[:-1], refs[-1]
    count = len(payloads) + 1
    _, blocks, length, _ = driven.shape
    for d in range(2):
        features = here[d] + there[d]
        key = features[:, :STATE]
        square = jnp.sum(key * key, axis=1, keepdims=True)
        low = features[:, 2 * STATE :].astype(jnp.bfloat16)
        for b in range(blocks):
            lanes = slice(b * LANES, (b + 1) * LANES)
            step = jnp.dot(low, step_weight[d, :, lanes], preferred_element_type=jnp.float32)
            beta = 2.0 * rate[d : d + 1, lanes] / (1.0 + jnp.exp(-step))
            value = beta / (1.0 + beta * square)
            eps[d, pl.ds(b, length, stride=blocks)] = value
            drive[d, pl.ds(b, length, stride=blocks)] = value * driven[d, b].astype(jnp.float32)
        spread(keys, features, 0)

        def body(t, carry):
            products, states = carry
            at = pl.ds(pl.multiple_of(t * blocks, blocks), blocks)
            e, x = eps[d, at], drive[d, at]
            new_products, new_states = [], []
            for n in range(STATE):
                k = row(keys, n, t, blocks)
                decay = 1.0 - e * (k * k)
                new_products.append(products[n] * decay)
                new_states.append(states[n] * decay + k * x)
            return tuple(new_products), tuple(new_states)

        one = tuple(jnp.ones((blocks, LANES), jnp.float32) for _ in range(STATE))
        zero = tuple(jnp.zeros((blocks, LANES), jnp.float32) for _ in range(STATE))
        products, states = steps(length, d == 1, body, (one, zero))
        for shift, payload in enumerate(payloads, 1):

            @pl.when((place[0] + shift < count) == (d == 0))
            def _():
                for n in range(STATE):
                    payload[0, n] = products[n].astype(payload.dtype)
                    payload[1, n] = states[n].astype(payload.dtype)


def entering(place, slots, d):
    count = len(slots) + 1
    states, passed = None, None
    for distance in range(1, count):
        slot = slots[distance - 1] if d == 0 else slots[count - distance - 1]
        reached = place[0] >= distance if d == 0 else place[0] + distance < count
        new = []
        for n in range(STATE):
            value = slot[1, n].astype(jnp.float32)
            if passed is not None:
                value = passed[n] * value
            value = jnp.where(reached, value, 0.0)
            new.append(value if states is None else states[n] + value)
        states = new
        if distance + 1 < count:
            factor = [slot[0, n].astype(jnp.float32) for n in range(STATE)]
            passed = factor if passed is None else [p * f for p, f in zip(passed, factor)]
    return tuple(states)


def read_scan(place, driven, here, there, eps, drive, gate, skip, slots, out, keys, queries, total):
    _, blocks, length, _ = driven.shape
    for d in range(2):
        features = here[d] + there[d]
        spread(keys, features, 0)
        spread(queries, features, STATE)

        def body(t, states):
            at = pl.ds(pl.multiple_of(t * blocks, blocks), blocks)
            e, x = eps[d, at], drive[d, at]
            new_states = []
            reads = [None] * 4
            for n in range(STATE):
                k = row(keys, n, t, blocks)
                q = row(queries, n, t, blocks)
                state = states[n] * (1.0 - e * (k * k)) + k * x
                new_states.append(state)
                part = q * state
                reads[n % 4] = part if reads[n % 4] is None else reads[n % 4] + part
            read = (reads[0] + reads[1]) + (reads[2] + reads[3])
            total[at] = read if d == 0 else total[at] + read
            return tuple(new_states)

        steps(length, d == 1, body, entering(place, slots, d))
    for b in range(blocks):
        lanes = slice(b * LANES, (b + 1) * LANES)
        g = gate[b].astype(jnp.float32)
        reads = total[pl.ds(b, length, stride=blocks)]
        for d in range(2):
            reads = reads + skip[d : d + 1, lanes] * driven[d, b].astype(jnp.float32)
        out[:, lanes] = (reads * (g / (1.0 + jnp.exp(-g)))).astype(jnp.bfloat16)


def read_kernel(place, driven, here, there, eps, drive, gate, skip, *refs):
    slots, (out, keys, queries, total) = refs[:-4], refs[-4:]
    read_scan(
        place, driven, here, there, eps, drive, gate, skip, slots, out, keys, queries, total
    )


def mix_kernel(place, driven, here, there, eps, drive, gate, skip, *refs):
    kept, sent, keys, queries, total, combined, local, arrived = refs[-8:]
    count = local.shape[0]
    slots, weights = refs[: -8 - count], refs[-8 - count : -8]
    columns = local.shape[2]
    shares = kept.shape[2] // columns
    copies = [
        pltpu.make_async_copy(weight, local.at[j], arrived.at[j])
        for j, weight in enumerate(weights)
    ]
    for copy in copies:
        copy.start()
    read_scan(
        place, driven, here, there, eps, drive, gate, skip, slots, combined, keys, queries, total
    )
    for j, copy in enumerate(copies):
        copy.wait()
        source = place[0] ^ j
        slot = (source // shares) ^ place[1]
        lanes = pl.ds(pl.multiple_of(source % shares * columns, LANES), columns)
        value = jnp.dot(combined[...], local[j], preferred_element_type=jnp.float32)

        @pl.when(slot % 2 == 0)
        def _():
            kept[slot // 2, :, lanes] = value

        @pl.when(slot % 2 == 1)
        def _():
            sent[slot // 2, :, lanes] = value


def kernel(body, args, shapes, scratch, remote=0):
    def space(at, arg):
        if arg.dtype == jnp.int32:
            return pltpu.SMEM
        return pl.ANY if at >= len(args) - remote else pltpu.VMEM

    return pl.pallas_call(
        body,
        out_shape=[jax.ShapeDtypeStruct(shape, dtype) for shape, dtype in shapes],
        in_specs=[
            pl.BlockSpec(memory_space=space(at, arg)) for at, arg in enumerate(args)
        ],
        out_specs=[pl.BlockSpec(memory_space=pltpu.VMEM) for _ in shapes],
        scratch_shapes=[
            pltpu.SemaphoreType.DMA(shape) if dtype is None else pltpu.VMEM(shape, dtype)
            for shape, dtype in scratch
        ],
    )(*args)


def swapped(own, axis, stop, scale):
    held = {0: own}
    distance = stop // 2
    while distance:
        for at in sorted(held):
            held[at + distance] = swap(held[at], axis, scale * distance)
        distance //= 2
    return [held[at] for at in range(stop)]


def beside(far):
    return [part for one in far for part in (one, swap(one, "seq", 1))]


def place():
    return jnp.stack([lax.axis_index("seq"), lax.axis_index("chan")]).astype(jnp.int32)


def exchanged_projection(hidden_in, norm_gain, in_weight):
    seq, chan = lax.axis_size("seq"), lax.axis_size("chan")
    slots = seq // 2
    length, columns = hidden_in.shape
    rows, _, channels = in_weight.shape
    share = channels // slots
    group = lax.axis_index("seq") // 2

    def piece(at):
        part = lax.dynamic_slice_in_dim(in_weight, at * share, share, 2)
        return part.reshape(rows, 2 * share)

    edge = WIDTH - 1
    edges = jnp.concatenate(
        [hidden_in[:edge], hidden_in[-edge:], jnp.zeros((EDGE - 2 * edge, columns), jnp.bfloat16)]
    )
    own = jnp.concatenate([hidden_in, swap(edges, "seq", 1)])
    hidden = [own] + [swap(own, "seq", 2 * k) for k in range(1, slots)]
    weights = [piece(group)] + [swap(piece(group ^ k), "seq", 2 * k) for k in range(1, slots)]
    weights = beside(weights)
    hidden = swapped(jnp.stack(hidden), "chan", chan, 1)
    projected = kernel(
        project_kernel,
        (place(), norm_gain.reshape(chan, 1, columns), *hidden, *weights),
        [((2, share // LANES, length + EDGE, LANES), jnp.bfloat16)] * slots,
        [
            ((chan * columns // rows, slots * (length + EDGE), rows), jnp.bfloat16),
            ((slots, share // LANES, EDGE, LANES), jnp.float32),
        ],
    )
    return [projected[0]] + [swap(projected[k], "seq", 2 * k) for k in range(1, slots)]


def gathered_projection(hidden_in, norm_gain, in_weight):
    gathered = lax.all_gather(hidden_in, "chan", axis=1, tiled=True).astype(jnp.float32)
    normed = (
        gathered
        * lax.rsqrt(jnp.mean(gathered * gathered, axis=1, keepdims=True) + 1e-05)
        * norm_gain[None, :]
    ).astype(jnp.bfloat16)
    length = normed.shape[0]
    channels = in_weight.shape[2]
    piece = lax.all_gather(in_weight, "seq", axis=0, tiled=True)
    projected = jnp.dot(
        normed, piece.reshape(piece.shape[0], 2 * channels), preferred_element_type=jnp.float32
    ).astype(jnp.bfloat16)
    projected = projected.reshape(length, 2, channels // LANES, LANES).transpose(1, 2, 0, 3)
    branch = with_edges(projected[0], "seq", WIDTH - 1)
    gate = jnp.pad(projected[1], ((0, 0), (0, EDGE), (0, 0)))
    return [jnp.stack([branch, gate])]


def power(count):
    return count & (count - 1) == 0


def exchanged(payloads):
    count = lax.axis_size("seq")
    slots = []
    for shift, payload in enumerate(payloads, 1):
        pairs = [(i, (i + shift) % count) for i in range(count)]
        slots.append(lax.ppermute(payload, "seq", pairs))
    return slots


def summed(kept, sent):
    distance = 1
    parts = kept + swap(sent, "chan", distance)
    while parts.shape[0] > 1:
        distance *= 2
        received = swap(parts[1::2].astype(jnp.bfloat16), "chan", distance)
        parts = parts[::2] + received.astype(jnp.float32)
    return parts[0].astype(jnp.bfloat16)


def gathered_mix(combined, out_weight):
    partial = jnp.dot(
        combined,
        lax.all_gather(out_weight, "seq", axis=1, tiled=True),
        preferred_element_type=jnp.float32,
    )
    summed = lax.psum(partial, "chan")
    share = summed.shape[1] // lax.axis_size("chan")
    part = lax.dynamic_slice_in_dim(summed, lax.axis_index("chan") * share, share, 1)
    return part.astype(jnp.bfloat16)


def shard(
    hidden_in,
    norm_gain,
    in_weight,
    conv_weight,
    conv_bias,
    proj_weight,
    step_weight,
    decay_rate,
    skip_gain,
    out_weight,
):
    seq, chan = lax.axis_size("seq"), lax.axis_size("chan")
    length, columns = hidden_in.shape
    rows, _, channels = in_weight.shape
    blocks = channels // LANES
    exchange = (
        power(seq)
        and power(chan)
        and chan > 1
        and 2 * channels % (seq * LANES) == 0
        and columns % rows == 0
        and rows % LANES == 0
        and seq % chan == 0
    )
    project = exchanged_projection if exchange else gathered_projection
    slots = project(hidden_in, norm_gain, in_weight)
    tail = (blocks, LANES)
    bf16, f32 = jnp.bfloat16, jnp.float32
    driven, gate, features = kernel(
        conv_kernel,
        (
            lax.axis_index("seq").reshape(1).astype(jnp.int32),
            conv_weight,
            conv_bias,
            proj_weight,
            *slots,
        ),
        [
            ((2, blocks, length, LANES), bf16),
            ((blocks, length, LANES), bf16),
            ((2, length, proj_weight.shape[2]), f32),
        ],
        [((length + 16, LANES), f32)],
    )
    distance = 1
    there = jnp.zeros_like(features)
    while distance < chan:
        features = features + there
        there = swap(features, "chan", distance)
        distance *= 2
    spread_shape = ((STATE, length, LANES), f32)
    at = place()
    eps, drive, *payloads = kernel(
        summary_kernel,
        (at, driven, features, there, step_weight, decay_rate),
        [((2, length * blocks, LANES), f32)] * 2 + [((2, STATE, *tail), bf16)] * (seq - 1),
        [spread_shape],
    )
    held = exchanged(payloads)
    common = (at, driven, features, there, eps, drive, gate, skip_gain, *held)
    scratch = [spread_shape] * 2 + [((length * blocks, LANES), f32)]
    if not exchange:
        (combined,) = kernel(read_kernel, common, [((length, channels), bf16)], scratch)
        return gathered_mix(combined, out_weight)
    width = out_weight.shape[1]
    outs = beside(swapped(out_weight, "seq", seq // 2, 2))
    kept, sent = kernel(
        mix_kernel,
        (*common, *outs),
        [((chan // 2, length, seq // chan * width), f32)] * 2,
        [
            *scratch,
            ((length, channels), bf16),
            ((seq, channels, width), bf16),
            ((seq,), None),
        ],
        seq,
    )
    return summed(kept, sent)


def solution(mesh):
    in_specs = (
        P("seq", "chan"),
        P(),
        P("seq", None, "chan"),
        P(None, None, "chan"),
        P(None, "chan"),
        P(None, "chan", None),
        P(None, None, "chan"),
        P(None, "chan"),
        P(None, "chan"),
        P("chan", "seq"),
    )
    out_specs = P("seq", "chan")
    return jax.shard_map(shard, mesh=mesh, in_specs=in_specs, out_specs=out_specs, check_vma=False)
```
